32 devices in a mesh: cohort: 2 (over y), bx: 16 (over z, x, core).
Axes of the slice: x: 2, y: 2, z: 4, core: 2. Of those that a mesh axis runs over, the one named last changes fastest.
Arguments:
- bold: bfloat16 [256, 12, 4096], P('cohort', None, 'bx'), parts along dimension 0, may hold values from -6 to 6
- nbr_table: int32 [256, 4096], P('cohort', 'bx'), parts along dimension 0, may hold values from -1 to 767, as said below
- subject: int32 [256], P('cohort'), parts along dimension 0, may hold values from 0 to 7
Outputs:
- spread: float32 [8192], P(('cohort', 'bx')), parts along dimension 0
- gram_mean: float32 [256, 128], P('cohort'), parts along dimension 0
The draws below stay inside these ranges and needn't reach their ends.
There are 2 independent parts, one for each index of `cohort`. The reference program is written for one: setup_inputs(seed, part) draws one part's arguments, and reference() takes and returns one part's arrays. A program takes and returns all parts, laid end to end along the dimension named above; each array names one. Nothing has to cross between parts.
Inputs may be any that keep to these rules, and one draw needn't show every extreme that they name: `nbr_table`: rows 125 to 127 are all -1 and row (124) // 2 names the centre itself (256 + its place in its block). Any other entry is -1 or the place, in the window made of the previous block, the centre's own block and the next block (768 voxels in order), of a voxel at most 147 voxels away from the centre in voxel order; no entry names a voxel outside the cohort's 4096 voxels.
All inputs are finite; a program needn't handle non-finite values.
Results may differ from the reference program's by a relative error of at most 0.0003.
Values may be sent and summed in bfloat16 or wider, within the bound.
A program may use at most 64 MiB of HBM per device.

```python
import jax
import jax.numpy as jnp
from jax import lax

VB = 256
E = 128
TP = 12
NB = 125
NBP = 128
SUBJ = 8
ROW = 8
PLANE = 64
NVOX = 4096
N_BX = 16


def draw_nbr_table(key, part):
    member = jnp.arange(NB, dtype=jnp.int32)
    along_x = member // 25 - 2
    along_y = member // 5 % 5 - 2
    along_z = member % 5 - 2
    base_offset = along_x * PLANE + along_y * ROW + along_z
    is_centre = (member == (NB - 1) // 2)[:, None]
    subkeys = jax.random.split(key, 2)
    jitter = jax.random.randint(subkeys[0], (NB, NVOX), -1, 2).astype(jnp.int32)
    jitter = jnp.where(is_centre, 0, jitter)
    keeping = jax.random.randint(subkeys[1], (NB, NVOX), 0, 4) > 0
    keeping = keeping | is_centre
    centre_ids = jnp.arange(NVOX, dtype=jnp.int32)[None, :]
    target = centre_ids + base_offset[:, None] + jitter
    inside = keeping & (target >= 0) & (target < NVOX)
    local_place = target - (centre_ids // VB - 1) * VB
    table = jnp.where(inside, local_place, -1).astype(jnp.int32)
    padding = jnp.full((NBP - NB, NVOX), -1, jnp.int32)
    return jnp.concatenate([table, padding], axis=0)


def plant(array, rng, least, top_value):
    shape = array.shape
    index_at = [jax.random.randint(jax.random.fold_in(rng, axis), (), 0, shape[axis]) for axis in range(len(shape))]
    array = array.at[tuple(index_at)].set(least)
    longest = shape.index(max(shape))
    index_at[longest] = (index_at[longest] + 1) % shape[longest]
    return array.at[tuple(index_at)].set(top_value)


def levels(rng, extent, cuts, low, top_value):
    gain = 1.0
    for dim, shards_of in cuts:
        heights = jax.random.uniform(jax.random.fold_in(jax.random.fold_in(rng, 6), dim), (shards_of,), jnp.float32, low / len(cuts), top_value / len(cuts))
        gain = gain * jnp.repeat(jnp.exp(heights), extent[dim] // shards_of).reshape((-1,) + (1,) * (len(extent) - 1 - dim))
    return gain


def normal_values(rng, dims, scale, limit, shards=(), held_as=jnp.bfloat16):
    values = jax.random.normal(rng, dims, jnp.float32) * scale
    if len(shards) > 0:
        values = levels(rng, dims, shards, -0.22, 0.18) * values
    return jnp.clip(values, min=-limit, max=limit).astype(held_as)


def setup_inputs(seed: int = 0, part: int = 0) -> dict:
    key_list = jax.random.split(jax.random.key(seed), 4)
    part_keys = jax.random.split(jax.random.fold_in(key_list[3], part), 4)
    bold = normal_values(part_keys[0], (E, TP, NVOX), 1.0, 6.0, ((2, 16),))
    nbr_table = draw_nbr_table(jax.random.fold_in(jax.random.fold_in(key_list[3], part), 71), part)
    subject = plant(jax.random.randint(part_keys[2], (E,), 0, SUBJ), jax.random.fold_in(part_keys[2], 1), 0, SUBJ - 1).astype(jnp.int32)
    return dict(bold=bold, nbr_table=nbr_table, subject=subject)


VARIANCE_FLOOR = 0.05

def normalize(series):
    values = series.astype(jnp.float32)
    centred = values - lax.optimization_barrier(jnp.mean(values, axis=1, keepdims=True))
    divisor = jnp.sqrt(lax.optimization_barrier(jnp.sum(centred * centred, axis=1, keepdims=True)) + 1.0)
    return (centred / divisor).astype(jnp.bfloat16)

def zscore(correl, onehot, counts):
    averages = jnp.einsum('es,ecj->scj', onehot, correl, precision=lax.Precision.HIGHEST) / counts[:, None, None]
    expanded = jnp.einsum('es,scj->ecj', onehot, averages, precision=lax.Precision.HIGHEST)
    deviation = correl - expanded
    variance = jnp.einsum('es,ecj->scj', onehot, deviation * deviation, precision=lax.Precision.HIGHEST) / counts[:, None, None]
    divisor = jnp.einsum('es,scj->ecj', onehot, jnp.sqrt(variance + VARIANCE_FLOOR), precision=lax.Precision.HIGHEST)
    return deviation / divisor

def reference(bold, nbr_table, subject):
    normed = normalize(bold).astype(jnp.float32)
    onehot = (subject[:, None] == jnp.arange(SUBJ, dtype=jnp.int32)[None, :]).astype(jnp.float32)
    counts = jnp.maximum(lax.optimization_barrier(jnp.sum(onehot, axis=0)), 1.0)
    padded = jnp.pad(normed, ((0, 0), (0, 0), (VB, VB)))

    def one_block(block_id):
        first_col = (block_id * VB).astype(jnp.int32)
        lookup = lax.dynamic_slice_in_dim(nbr_table, first_col, VB, 1)
        usable = (lookup >= 0).T
        position = (jnp.where(lookup >= 0, lookup, 0) + first_col).T.reshape(-1).astype(jnp.int32)
        centre = lax.dynamic_slice_in_dim(normed, first_col, VB, 2)
        gathered = jnp.take(padded, position, axis=2).reshape(E, TP, VB, NBP)
        correl = jnp.einsum('etc,etcj->ecj', centre, gathered, precision=lax.Precision.HIGHEST)
        correl = jnp.where(usable[None], correl, jnp.float32(0.0))
        features = zscore(correl, onehot, counts)
        kernel = jnp.einsum('ecj,fcj->cef', features, features, precision=lax.Precision.HIGHEST) / NB
        return (lax.optimization_barrier(jnp.sum(kernel, axis=0)), jnp.sqrt(lax.optimization_barrier(jnp.sum(kernel * kernel, axis=(1, 2))) / E))
    block_sums, spreads = lax.map(one_block, jnp.arange(N_BX).astype(jnp.int32))
    return (spreads.reshape(-1), lax.optimization_barrier(jnp.sum(block_sums, axis=0)) / NVOX)
```

```python
import functools

import jax
import jax.numpy as jnp
from jax import lax
from jax.experimental import pallas as pl
from jax.experimental.pallas import tpu as pltpu
from jax.sharding import PartitionSpec as P

NB = 125
SUBJ = 8
REACH = 147
VARIANCE_FLOOR = 0.05

SLOTS = 16
GROUP = 16
CHUNK = 64
LANES = 128
LEAD = 160
SPAN = 384


def normalize(series):
    values = series.astype(jnp.float32)
    centred = values - jnp.mean(values, axis=1, keepdims=True)
    divisor = jnp.sqrt(jnp.sum(centred * centred, axis=1, keepdims=True) + 1.0)
    return (centred / divisor).astype(jnp.bfloat16)


def features_kernel(win_ref, own_ref, idx_ref, sid_ref, hot_ref, inv_ref, keep_ref,
                    square_ref, gram_ref, lhs_ref, prod_ref, mean_ref):
    chunk = pl.program_id(0)
    first = chunk * CHUNK
    parity = lax.rem(chunk, 2)
    start = pl.multiple_of((chunk // 2) * LANES, LANES)
    epochs = gram_ref.shape[0]
    depth = GROUP * SLOTS
    groups = epochs // GROUP

    row_epoch = lax.broadcasted_iota(jnp.int32, (GROUP, depth), 0)
    col_epoch = lax.broadcasted_iota(jnp.int32, (GROUP, depth), 1) // SLOTS
    diagonal = row_epoch == col_epoch

    @pl.when(chunk == 0)
    def _():
        gram_ref[...] = jnp.zeros_like(gram_ref)

    def one_group(g, carry):
        cols = pl.ds(pl.multiple_of(g * depth, depth), depth)
        for c in range(CHUNK):
            row = jnp.broadcast_to(own_ref[pl.ds(first + c, 1), cols], (GROUP, depth))
            lhs_ref[c * GROUP:(c + 1) * GROUP, :] = jnp.where(diagonal, row, 0.0).astype(jnp.bfloat16)
        prod = jnp.dot(lhs_ref[...], win_ref[parity, cols, pl.ds(start, SPAN)],
                       preferred_element_type=jnp.float32)
        prod_ref[:, pl.ds(pl.multiple_of(g * GROUP, GROUP), GROUP), :] = prod.reshape(CHUNK, GROUP, SPAN)
        for c in range(CHUNK // 2):
            pair = []
            for i in range(2):
                row = jnp.broadcast_to(own_ref[pl.ds(first + 2 * c + i, 1), cols], (SUBJ, depth))
                pair.append(row * keep_ref[:, cols])
            lhs_ref[c * GROUP:(c + 1) * GROUP, :] = jnp.concatenate(pair, axis=0).astype(jnp.bfloat16)
        part = jnp.dot(lhs_ref[:CHUNK * SUBJ, :], win_ref[parity, cols, pl.ds(start, SPAN)],
                       preferred_element_type=jnp.float32).reshape(CHUNK, SUBJ, SPAN)

        @pl.when(g == 0)
        def _():
            mean_ref[...] = part

        @pl.when(g > 0)
        def _():
            mean_ref[...] += part
        return carry

    lax.fori_loop(0, groups, one_group, 0)

    inv = inv_ref[...]

    def select(ref, c, lane, tile, rows):
        out = jnp.zeros((rows, LANES), jnp.float32)
        at = jnp.broadcast_to(lane, (rows, LANES))
        for t in range(SPAN // LANES):
            got = jnp.take_along_axis(ref[c, :, t * LANES:(t + 1) * LANES], at, axis=1,
                                      mode="promise_in_bounds")
            out = jnp.where(jnp.broadcast_to(tile == t, (rows, LANES)), got, out)
        return out

    def expand(stat):
        return jnp.concatenate(
            [jnp.take_along_axis(stat, sid_ref[r * 8:(r + 1) * 8, :], axis=0, mode="promise_in_bounds")
             for r in range(epochs // 8)], axis=0)

    def one_pair(p, carry):
        devs, sqs = [], []
        for i in range(2):
            c = 2 * p + i
            raw = idx_ref[pl.ds(first + c, 1), :]
            local = raw - (2 * LANES + first - LEAD)
            lane = local & (LANES - 1)
            tile = jnp.where(raw < 0, -1, local >> 7)
            correl = select(prod_ref, c, lane, tile, epochs)
            mean = select(mean_ref, c, lane, tile, SUBJ) * inv
            dev = correl - expand(mean)
            devs.append(dev)
            sqs.append((dev * dev).astype(jnp.bfloat16))
        var = jnp.dot(hot_ref[...], jnp.concatenate(sqs, axis=1), preferred_element_type=jnp.float32)[:SUBJ]
        total = None
        for i in range(2):
            scale = lax.rsqrt(var[:, i * LANES:(i + 1) * LANES] * inv + VARIANCE_FLOOR)
            feat = (devs[i] * expand(scale)).astype(jnp.bfloat16)
            kern = lax.dot_general(feat, feat, (((1,), (1,)), ((), ())), preferred_element_type=jnp.float32)
            square_ref[pl.ds(first + 2 * p + i, 1), :] = jnp.sum(kern * kern, axis=0, keepdims=True)
            total = kern if total is None else total + kern
        gram_ref[...] += total
        return carry

    lax.fori_loop(0, CHUNK // 2, one_pair, 0)


def per_device(bold, nbr_table, subject):
    epochs, points, block_len = bold.shape
    count = lax.axis_size("bx")
    normed = jnp.pad(normalize(bold), ((0, 0), (0, SLOTS - points), (0, 0)))
    left = lax.ppermute(normed[:, :, block_len - LEAD:], "bx", [(i, i + 1) for i in range(count - 1)])
    right = lax.ppermute(normed[:, :, :LEAD], "bx", [(i + 1, i) for i in range(count - 1)])
    ext = jnp.concatenate([left, normed, right], axis=2).reshape(epochs * SLOTS, -1)
    wide = SPAN + LANES
    win = jnp.stack([ext[:, :wide], ext[:, CHUNK:CHUNK + wide]])
    own = normed.reshape(epochs * SLOTS, block_len).T.astype(jnp.float32)
    onehot = subject[None, :] == jnp.arange(SUBJ, dtype=jnp.int32)[:, None]
    counts = jnp.maximum(jnp.sum(onehot.astype(jnp.float32), axis=1), 1.0)
    inv = jnp.broadcast_to((1.0 / counts)[:, None], (SUBJ, LANES))
    sid = jnp.broadcast_to(subject[:, None], (epochs, LANES))
    hot = jnp.pad(onehot.astype(jnp.bfloat16), ((0, 8), (0, 0)))
    keep = jnp.repeat(onehot.astype(jnp.float32), SLOTS, axis=1)
    vmem = pl.BlockSpec(memory_space=pltpu.VMEM)
    squares, total = pl.pallas_call(
        features_kernel,
        grid=(block_len // CHUNK,),
        in_specs=[vmem] * 7,
        out_specs=[vmem] * 2,
        out_shape=[jax.ShapeDtypeStruct((block_len, epochs), jnp.float32),
                   jax.ShapeDtypeStruct((epochs, epochs), jnp.float32)],
        scratch_shapes=[
            pltpu.VMEM((CHUNK * GROUP, GROUP * SLOTS), jnp.bfloat16),
            pltpu.VMEM((CHUNK, epochs, SPAN), jnp.float32),
            pltpu.VMEM((CHUNK, SUBJ, SPAN), jnp.float32),
        ],
        compiler_params=pltpu.CompilerParams(dimension_semantics=("arbitrary",),
                                             vmem_limit_bytes=60 * 1024 * 1024),
        name="features",
    )(win, own, nbr_table.T, sid, hot, inv, keep)
    spread = jnp.sqrt(jnp.sum(squares, axis=1) / (epochs * NB * NB))
    gram_mean = lax.psum(total, "bx") / (NB * block_len * count)
    return spread, gram_mean


def solution(mesh):
    return jax.shard_map(
        per_device,
        mesh=mesh,
        in_specs=(P("cohort", None, "bx"), P("cohort", "bx"), P("cohort")),
        out_specs=(P(("cohort", "bx")), P("cohort", None)),
        check_vma=False,
    )
```

```python
import functools

import jax
import jax.numpy as jnp
from jax import lax
from jax.experimental import pallas as pl
from jax.experimental.pallas import tpu as pltpu
from jax.sharding import PartitionSpec as P

NB = 125
SUBJ = 8
REACH = 147
VARIANCE_FLOOR = 0.05

SLOTS = 16
GROUP = 16
CHUNK = 64
LANES = 128
LEAD = 160
SPAN = 384
BATCH = 4
MESH = pl.DeviceIdType.MESH


def normalize(series):
    values = series.astype(jnp.float32)
    centred = values - jnp.mean(values, axis=1, keepdims=True)
    divisor = jnp.sqrt(jnp.sum(centred * centred, axis=1, keepdims=True) + 1.0)
    return (centred / divisor).astype(jnp.bfloat16)


def features_kernel(win_ref, own_ref, idx_ref, sid_ref, hot_ref, inv_ref, keep_ref,
                    square_ref, gram_ref, lhs_ref, prod_ref, mean_ref, root_ref, sq_ref, feat_ref, var_ref):
    chunk = pl.program_id(0)
    first = chunk * CHUNK
    parity = lax.rem(chunk, 2)
    start = pl.multiple_of((chunk // 2) * LANES, LANES)
    epochs = gram_ref.shape[0]
    depth = GROUP * SLOTS
    groups = epochs // GROUP

    row_epoch = lax.broadcasted_iota(jnp.int32, (GROUP, depth), 0)
    col_epoch = lax.broadcasted_iota(jnp.int32, (GROUP, depth), 1) // SLOTS
    diagonal = row_epoch == col_epoch

    @pl.when(chunk == 0)
    def _():
        gram_ref[...] = jnp.zeros_like(gram_ref)
        slots, block_len = idx_ref.shape
        for half in range(block_len // LANES):
            place = lax.broadcasted_iota(jnp.int32, (1, LANES), 1) + half * LANES
            shift = block_len - LEAD + place // CHUNK * CHUNK

            def one_tile(w, carry):
                at = lax.broadcasted_iota(jnp.int32, (32, LANES), 0) + w * 32
                hits = jnp.zeros((32, LANES), jnp.float32)
                for j in range(NB):
                    rel = idx_ref[j:j + 1, half * LANES:(half + 1) * LANES] - shift
                    hits = hits + jnp.where(jnp.broadcast_to(rel, (32, LANES)) == at, 1.0, 0.0)
                lhs = jnp.sqrt(hits)
                mean_ref[pl.ds(w * 4, 4), :, :LANES] = lhs.reshape(4, 8, LANES)
                return carry

            lax.fori_loop(0, SPAN // 32, one_tile, 0)
            for t in range(SPAN // LANES):
                tile = mean_ref[t * 16:(t + 1) * 16, :, :LANES].reshape(LANES, LANES)
                root_ref[half * LANES:(half + 1) * LANES, t * LANES:(t + 1) * LANES] = tile.T

    def one_group(g, carry):
        cols = pl.ds(pl.multiple_of(g * depth, depth), depth)
        for c in range(CHUNK):
            row = jnp.broadcast_to(own_ref[pl.ds(first + c, 1), cols], (GROUP, depth))
            lhs_ref[c * GROUP:(c + 1) * GROUP, :] = jnp.where(diagonal, row, 0.0).astype(jnp.bfloat16)
        prod = jnp.dot(lhs_ref[...], win_ref[parity, cols, pl.ds(start, SPAN)],
                       preferred_element_type=jnp.float32)
        prod_ref[:, pl.ds(pl.multiple_of(g * GROUP, GROUP), GROUP), :] = prod.reshape(CHUNK, GROUP, SPAN)
        for c in range(CHUNK // 2):
            pair = []
            for i in range(2):
                row = jnp.broadcast_to(own_ref[pl.ds(first + 2 * c + i, 1), cols], (SUBJ, depth))
                pair.append(row * keep_ref[:, cols])
            lhs_ref[c * GROUP:(c + 1) * GROUP, :] = jnp.concatenate(pair, axis=0).astype(jnp.bfloat16)
        part = jnp.dot(lhs_ref[:CHUNK * SUBJ, :], win_ref[parity, cols, pl.ds(start, SPAN)],
                       preferred_element_type=jnp.float32).reshape(CHUNK, SUBJ, SPAN)

        @pl.when(g == 0)
        def _():
            mean_ref[...] = part

        @pl.when(g > 0)
        def _():
            mean_ref[...] += part
        return carry

    lax.fori_loop(0, groups, one_group, 0)

    inv = jnp.concatenate([inv_ref[...]] * (SPAN // LANES), axis=1)
    feat_ref[...] = jnp.zeros_like(feat_ref)
    steps = CHUNK // BATCH

    def expand(stat, r):
        at = sid_ref[r * 8:(r + 1) * 8, :]
        return jnp.concatenate(
            [jnp.take_along_axis(stat[:, t * LANES:(t + 1) * LANES], at, axis=0, mode="promise_in_bounds")
             for t in range(SPAN // LANES)], axis=1)

    def one_batch(p, carry):
        base_c = jnp.maximum(p - 2, 0) * BATCH
        base_b = jnp.clip(p - 1, 0, steps - 1) * BATCH
        base_a = jnp.minimum(p, steps - 1) * BATCH
        total = None
        for i in range(BATCH):
            feat = feat_ref[i]
            kern = lax.dot_general(feat, feat, (((1,), (1,)), ((), ())), preferred_element_type=jnp.float32)
            square_ref[pl.ds(first + base_c + i, 1), :] = jnp.sum(kern * kern, axis=0, keepdims=True)
            total = kern if total is None else total + kern
        gram_ref[...] += total
        for i in range(BATCH):
            scale = lax.rsqrt(var_ref[i] * inv + VARIANCE_FLOOR) * root_ref[pl.ds(first + base_b + i, 1), :]
            scale = jnp.where(p > 0, scale, 0.0)
            for r in range(0, epochs // 8, 2):
                pair = [prod_ref[base_b + i, (r + k) * 8:(r + k + 1) * 8, :] * expand(scale, r + k) for k in range(2)]
                feat_ref[i, r * 8:(r + 2) * 8, :] = jnp.concatenate(pair, axis=0).astype(jnp.bfloat16)
        for i in range(BATCH):
            mean = mean_ref[base_a + i] * inv
            for r in range(0, epochs // 8, 2):
                pair = []
                for k in range(2):
                    rows = slice((r + k) * 8, (r + k + 1) * 8)
                    dev = prod_ref[base_a + i, rows, :] - expand(mean, r + k)
                    prod_ref[base_a + i, rows, :] = dev
                    pair.append(dev * dev)
                sq_ref[i, r * 8:(r + 2) * 8, :] = jnp.concatenate(pair, axis=0).astype(jnp.bfloat16)
            var_ref[i] = jnp.dot(hot_ref[...], sq_ref[i], preferred_element_type=jnp.float32)[:SUBJ]
        return carry

    lax.fori_loop(0, steps + 2, one_batch, 0)


def sum_kernel(count, part_ref, out_ref, took, send1, recv1, send2, recv2):
    me = lax.axis_index("bx")
    barrier = pltpu.get_barrier_semaphore()

    def greet(d, carry):
        pl.semaphore_signal(barrier, inc=1, device_id={"bx": lax.rem(me + d, count)}, device_id_type=MESH)
        return carry

    lax.fori_loop(1, count, greet, 0)
    pl.semaphore_wait(barrier, count - 1)

    def scatter(d):
        to = lax.rem(me + d, count)
        return pltpu.make_async_remote_copy(
            src_ref=part_ref.at[to], dst_ref=took.at[d], send_sem=send1.at[d], recv_sem=recv1.at[d],
            device_id={"bx": to}, device_id_type=MESH)

    def gather(d):
        return pltpu.make_async_remote_copy(
            src_ref=out_ref.at[me], dst_ref=out_ref.at[me], send_sem=send2.at[d], recv_sem=recv2.at[d],
            device_id={"bx": lax.rem(me + d, count)}, device_id_type=MESH)

    def landed(d):
        src = lax.rem(me + count - d, count)
        return pltpu.make_async_remote_copy(
            src_ref=out_ref.at[src], dst_ref=out_ref.at[src], send_sem=send2.at[d], recv_sem=recv2.at[d],
            device_id={"bx": lax.rem(me + d, count)}, device_id_type=MESH)

    def each(act):
        def body(d, carry):
            act(d)
            return carry
        lax.fori_loop(1, count, body, 0)

    each(lambda d: scatter(d).start())
    each(lambda d: scatter(d).wait_recv())

    def add(d, total):
        return total + took[d]

    out_ref[me] = lax.fori_loop(1, count, add, part_ref[me])
    each(lambda d: gather(d).start())
    each(lambda d: landed(d).wait_recv())
    each(lambda d: scatter(d).wait_send())
    each(lambda d: gather(d).wait_send())


def sum_over_bx(total):
    count = lax.axis_size("bx")
    rows, cols = total.shape
    blocks = total.reshape(count, rows // count, cols)
    vmem = pl.BlockSpec(memory_space=pltpu.VMEM)
    return pl.pallas_call(
        functools.partial(sum_kernel, count),
        in_specs=[vmem],
        out_specs=vmem,
        out_shape=jax.ShapeDtypeStruct(blocks.shape, jnp.float32),
        scratch_shapes=[pltpu.VMEM(blocks.shape, jnp.float32)] + [pltpu.SemaphoreType.DMA((count,))] * 4,
        compiler_params=pltpu.CompilerParams(collective_id=0, has_side_effects=True),
        name="sum_over_bx",
    )(blocks).reshape(rows, cols)


def per_device(bold, nbr_table, subject):
    epochs, points, block_len = bold.shape
    count = lax.axis_size("bx")
    normed = jnp.pad(normalize(bold), ((0, 0), (0, SLOTS - points), (0, 0)))
    left = lax.ppermute(normed[:, :, block_len - LEAD:], "bx", [(i, i + 1) for i in range(count - 1)])
    right = lax.ppermute(normed[:, :, :LEAD], "bx", [(i + 1, i) for i in range(count - 1)])
    ext = jnp.concatenate([left, normed, right], axis=2).reshape(epochs * SLOTS, -1)
    wide = SPAN + LANES
    win = jnp.stack([ext[:, :wide], ext[:, CHUNK:CHUNK + wide]])
    own = normed.reshape(epochs * SLOTS, block_len).T.astype(jnp.float32)
    onehot = subject[None, :] == jnp.arange(SUBJ, dtype=jnp.int32)[:, None]
    counts = jnp.maximum(jnp.sum(onehot.astype(jnp.float32), axis=1), 1.0)
    inv = jnp.broadcast_to((1.0 / counts)[:, None], (SUBJ, LANES))
    sid = jnp.broadcast_to(subject[:, None], (epochs, LANES))
    hot = jnp.pad(onehot.astype(jnp.bfloat16), ((0, 8), (0, 0)))
    keep = jnp.repeat(onehot.astype(jnp.float32), SLOTS, axis=1)
    vmem = pl.BlockSpec(memory_space=pltpu.VMEM)
    squares, total = pl.pallas_call(
        features_kernel,
        grid=(block_len // CHUNK,),
        in_specs=[vmem] * 7,
        out_specs=[vmem] * 2,
        out_shape=[jax.ShapeDtypeStruct((block_len, epochs), jnp.float32),
                   jax.ShapeDtypeStruct((epochs, epochs), jnp.float32)],
        scratch_shapes=[
            pltpu.VMEM((CHUNK * GROUP, GROUP * SLOTS), jnp.bfloat16),
            pltpu.VMEM((CHUNK, epochs, SPAN), jnp.float32),
            pltpu.VMEM((CHUNK, SUBJ, SPAN), jnp.float32),
            pltpu.VMEM((block_len, SPAN), jnp.float32),
            pltpu.VMEM((BATCH, epochs, SPAN), jnp.bfloat16),
            pltpu.VMEM((BATCH, epochs, SPAN), jnp.bfloat16),
            pltpu.VMEM((BATCH, SUBJ, SPAN), jnp.float32),
        ],
        compiler_params=pltpu.CompilerParams(dimension_semantics=("arbitrary",),
                                             vmem_limit_bytes=60 * 1024 * 1024),
        name="features",
    )(win, own, nbr_table, sid, hot, inv, keep)
    spread = jnp.sqrt(jnp.sum(squares, axis=1) / (epochs * NB * NB))
    gram_mean = sum_over_bx(total) / (NB * block_len * count)
    return spread, gram_mean


def solution(mesh):
    return jax.shard_map(
        per_device,
        mesh=mesh,
        in_specs=(P("cohort", None, "bx"), P("cohort", "bx"), P("cohort")),
        out_specs=(P(("cohort", "bx")), P("cohort", None)),
        check_vma=False,
    )
```

```python
import functools

import jax
import jax.numpy as jnp
from jax import lax
from jax.experimental import pallas as pl
from jax.experimental.pallas import tpu as pltpu
from jax.sharding import PartitionSpec as P

NB = 125
SUBJ = 8
REACH = 147
VARIANCE_FLOOR = 0.05

SLOTS = 16
GROUP = 16
CHUNK = 64
LANES = 128
LEAD = 160
SPAN = 384
BATCH = 4
MESH = pl.DeviceIdType.MESH
BY_ROW = lax.GatherDimensionNumbers(
    offset_dims=(), collapsed_slice_dims=(0,), start_index_map=(0,),
    operand_batching_dims=(1,), start_indices_batching_dims=(1,))


def normalized(raw):
    values = raw.astype(jnp.float32)
    points = values.shape[0]
    centred = values - jnp.sum(values, axis=0, keepdims=True) * (1.0 / points)
    return centred * (1.0 / jnp.sqrt(jnp.sum(centred * centred, axis=0, keepdims=True) + 1.0))


def prepare_kernel(idx_ref, bold_ref, root_ref, own_ref, hit_ref):
    slots, block_len = idx_ref.shape
    points, epochs, _ = bold_ref.shape
    depth = GROUP * SLOTS
    for half in range(block_len // LANES):
        place = lax.broadcasted_iota(jnp.int32, (1, LANES), 1) + half * LANES
        shift = block_len - LEAD + place // CHUNK * CHUNK

        def one_tile(w, carry):
            at = lax.broadcasted_iota(jnp.int32, (32, LANES), 0) + w * 32 + shift
            hits = jnp.zeros((32, LANES), jnp.float32)
            for j in range(NB):
                named = idx_ref[j:j + 1, half * LANES:(half + 1) * LANES]
                hits = jnp.where(jnp.broadcast_to(named, (32, LANES)) == at, hits + 1.0, hits)
            hit_ref[pl.ds(pl.multiple_of(w * 32, 32), 32), :] = jnp.sqrt(hits)
            return carry

        lax.fori_loop(0, SPAN // 32, one_tile, 0)
        for t in range(SPAN // LANES):
            root_ref[half * LANES:(half + 1) * LANES, t * LANES:(t + 1) * LANES] = (
                hit_ref[t * LANES:(t + 1) * LANES, :].T)

    def one_group(g, carry):
        rows = pl.ds(pl.multiple_of(g * GROUP, GROUP), GROUP)
        rounded = normalized(bold_ref[:, rows, :]).astype(jnp.bfloat16).astype(jnp.float32)
        flat = rounded.reshape(points * GROUP, block_len)
        flat = jnp.concatenate([flat, jnp.zeros((depth - points * GROUP, block_len), jnp.float32)], axis=0)
        own_ref[:, pl.ds(pl.multiple_of(g * depth, depth), depth)] = flat.T
        return carry

    lax.fori_loop(0, epochs // GROUP, one_group, 0)


def features_kernel(ext_ref, own_ref, root_ref, sid_ref, hot_ref, inv_ref, keep_ref,
                    square_ref, gram_ref, win_ref, lhs_ref, prod_ref, mean_ref, sq_ref, feat_ref, var_ref):
    chunk = pl.program_id(0)
    first = chunk * CHUNK
    parity = lax.rem(chunk, 2)
    start = pl.multiple_of((chunk // 2) * LANES, LANES)
    epochs = gram_ref.shape[0]
    depth = GROUP * SLOTS
    groups = epochs // GROUP

    row_epoch = lax.broadcasted_iota(jnp.int32, (GROUP, depth), 0)
    col_epoch = lax.broadcasted_iota(jnp.int32, (GROUP, depth), 1) % GROUP
    diagonal = row_epoch == col_epoch

    @pl.when(chunk == 0)
    def _():
        gram_ref[...] = jnp.zeros_like(gram_ref)
        points = ext_ref.shape[0]
        wide = win_ref.shape[2]
        filler = jnp.zeros((depth - points * GROUP, wide), jnp.bfloat16)

        def fill(g, carry):
            rows = pl.ds(pl.multiple_of(g * GROUP, GROUP), GROUP)
            cells = normalized(ext_ref[:, rows, :]).reshape(points * GROUP, -1)
            base = pl.multiple_of(g * depth, depth)
            for side in range(2):
                win_ref[side, pl.ds(base, points * GROUP), :] = (
                    cells[:, side * CHUNK:side * CHUNK + wide].astype(jnp.bfloat16))
                win_ref[side, pl.ds(base + points * GROUP, depth - points * GROUP), :] = filler
            return carry

        lax.fori_loop(0, groups, fill, 0)

    def one_group(g, carry):
        cols = pl.ds(pl.multiple_of(g * depth, depth), depth)
        for c in range(CHUNK):
            row = jnp.broadcast_to(own_ref[pl.ds(first + c, 1), cols], (GROUP, depth))
            lhs_ref[c * GROUP:(c + 1) * GROUP, :] = jnp.where(diagonal, row, 0.0).astype(jnp.bfloat16)
        prod = jnp.dot(lhs_ref[...], win_ref[parity, cols, pl.ds(start, SPAN)],
                       preferred_element_type=jnp.float32)
        prod_ref[:, pl.ds(pl.multiple_of(g * GROUP, GROUP), GROUP), :] = prod.reshape(CHUNK, GROUP, SPAN)
        for c in range(CHUNK // 2):
            pair = []
            for i in range(2):
                row = jnp.broadcast_to(own_ref[pl.ds(first + 2 * c + i, 1), cols], (SUBJ, depth))
                pair.append(row * keep_ref[:, cols])
            lhs_ref[c * GROUP:(c + 1) * GROUP, :] = jnp.concatenate(pair, axis=0).astype(jnp.bfloat16)
        part = jnp.dot(lhs_ref[:CHUNK * SUBJ, :], win_ref[parity, cols, pl.ds(start, SPAN)],
                       preferred_element_type=jnp.float32).reshape(CHUNK, SUBJ, SPAN)

        @pl.when(g == 0)
        def _():
            mean_ref[...] = part

        @pl.when(g > 0)
        def _():
            mean_ref[...] += part
        return carry

    lax.fori_loop(0, groups, one_group, 0)

    inv = jnp.concatenate([inv_ref[...]] * (SPAN // LANES), axis=1)
    feat_ref[...] = jnp.zeros_like(feat_ref)
    steps = CHUNK // BATCH

    def expand(stat, r):
        at = sid_ref[r * 8:(r + 1) * 8, :]
        return jnp.concatenate(
            [lax.gather(stat[:, t * LANES:(t + 1) * LANES], at[..., None], BY_ROW, (1, 1),
                        mode="promise_in_bounds")
             for t in range(SPAN // LANES)], axis=1)

    def one_batch(p, carry):
        base_c = jnp.maximum(p - 2, 0) * BATCH
        base_b = jnp.clip(p - 1, 0, steps - 1) * BATCH
        base_a = jnp.minimum(p, steps - 1) * BATCH
        total = None
        for i in range(BATCH):
            feat = feat_ref[i]
            kern = lax.dot_general(feat, feat, (((1,), (1,)), ((), ())), preferred_element_type=jnp.float32)
            square_ref[pl.ds(first + base_c + i, 1), :] = jnp.sum(kern * kern, axis=0, keepdims=True)
            total = kern if total is None else total + kern
        gram_ref[...] += total
        for i in range(BATCH):
            scale = lax.rsqrt(var_ref[i] * inv + VARIANCE_FLOOR) * root_ref[pl.ds(first + base_b + i, 1), :]
            scale = jnp.where(p > 0, scale, 0.0)
            for r in range(0, epochs // 8, 2):
                pair = [prod_ref[base_b + i, (r + k) * 8:(r + k + 1) * 8, :] * expand(scale, r + k) for k in range(2)]
                feat_ref[i, r * 8:(r + 2) * 8, :] = jnp.concatenate(pair, axis=0).astype(jnp.bfloat16)
        for i in range(BATCH):
            mean = mean_ref[base_a + i] * inv
            for r in range(0, epochs // 8, 2):
                pair = []
                for k in range(2):
                    rows = slice((r + k) * 8, (r + k + 1) * 8)
                    dev = prod_ref[base_a + i, rows, :] - expand(mean, r + k)
                    prod_ref[base_a + i, rows, :] = dev
                    pair.append(dev * dev)
                sq_ref[i, r * 8:(r + 2) * 8, :] = jnp.concatenate(pair, axis=0).astype(jnp.bfloat16)
            var_ref[i] = jnp.dot(hot_ref[...], sq_ref[i], preferred_element_type=jnp.float32)[:SUBJ]
        return carry

    lax.fori_loop(0, steps + 2, one_batch, 0)


def sum_kernel(count, scale, part_ref, out_ref, took, send1, recv1, send2, recv2):
    me = lax.axis_index("bx")
    barrier = pltpu.get_barrier_semaphore()

    def greet(d, carry):
        pl.semaphore_signal(barrier, inc=1, device_id={"bx": lax.rem(me + d, count)}, device_id_type=MESH)
        return carry

    lax.fori_loop(1, count, greet, 0)
    pl.semaphore_wait(barrier, count - 1)

    def scatter(d):
        to = lax.rem(me + d, count)
        return pltpu.make_async_remote_copy(
            src_ref=part_ref.at[to], dst_ref=took.at[d], send_sem=send1.at[d], recv_sem=recv1.at[d],
            device_id={"bx": to}, device_id_type=MESH)

    def gather(d):
        return pltpu.make_async_remote_copy(
            src_ref=out_ref.at[me], dst_ref=out_ref.at[me], send_sem=send2.at[d], recv_sem=recv2.at[d],
            device_id={"bx": lax.rem(me + d, count)}, device_id_type=MESH)

    def landed(d):
        src = lax.rem(me + count - d, count)
        return pltpu.make_async_remote_copy(
            src_ref=out_ref.at[src], dst_ref=out_ref.at[src], send_sem=send2.at[d], recv_sem=recv2.at[d],
            device_id={"bx": lax.rem(me + d, count)}, device_id_type=MESH)

    def each(act):
        def body(d, carry):
            act(d)
            return carry
        lax.fori_loop(1, count, body, 0)

    each(lambda d: scatter(d).start())
    each(lambda d: scatter(d).wait_recv())

    def add(d, total):
        return total + took[d]

    out_ref[me] = lax.fori_loop(1, count, add, part_ref[me]) * scale
    each(lambda d: gather(d).start())
    each(lambda d: landed(d).wait_recv())
    each(lambda d: scatter(d).wait_send())
    each(lambda d: gather(d).wait_send())


def sum_over_bx(total, scale):
    count = lax.axis_size("bx")
    rows, cols = total.shape
    blocks = total.reshape(count, rows // count, cols)
    vmem = pl.BlockSpec(memory_space=pltpu.VMEM)
    return pl.pallas_call(
        functools.partial(sum_kernel, count, scale),
        in_specs=[vmem],
        out_specs=vmem,
        out_shape=jax.ShapeDtypeStruct(blocks.shape, jnp.float32),
        scratch_shapes=[pltpu.VMEM(blocks.shape, jnp.float32)] + [pltpu.SemaphoreType.DMA((count,))] * 4,
        compiler_params=pltpu.CompilerParams(collective_id=0, has_side_effects=True),
        name="sum_over_bx",
    )(blocks).reshape(rows, cols)


def per_device(bold, nbr_table, subject):
    epochs, points, block_len = bold.shape
    count = lax.axis_size("bx")
    bold = bold.transpose(1, 0, 2)
    left = lax.ppermute(bold[:, :, block_len - LEAD:], "bx", [(i, i + 1) for i in range(count - 1)])
    right = lax.ppermute(bold[:, :, :LEAD], "bx", [(i + 1, i) for i in range(count - 1)])
    vmem = pl.BlockSpec(memory_space=pltpu.VMEM)
    wide = SPAN + LANES
    depth = GROUP * SLOTS
    span = epochs * SLOTS
    root, own = pl.pallas_call(
        prepare_kernel,
        in_specs=[vmem] * 2,
        out_specs=[vmem] * 2,
        out_shape=[jax.ShapeDtypeStruct((block_len, SPAN), jnp.float32),
                   jax.ShapeDtypeStruct((block_len, span), jnp.float32)],
        scratch_shapes=[pltpu.VMEM((SPAN, LANES), jnp.float32)],
        cost_estimate=pl.CostEstimate(flops=2 * 10 ** 9, bytes_accessed=4 * 10 ** 6, transcendentals=0),
        name="prepare",
    )(nbr_table, bold)
    ext = jnp.concatenate([left, bold, right], axis=2)
    onehot = subject[None, :] == jnp.arange(SUBJ, dtype=jnp.int32)[:, None]
    counts = jnp.maximum(jnp.sum(onehot.astype(jnp.float32), axis=1), 1.0)
    inv = jnp.broadcast_to((1.0 / counts)[:, None], (SUBJ, LANES))
    sid = jnp.broadcast_to(subject[:, None], (epochs, LANES))
    hot = jnp.pad(onehot.astype(jnp.bfloat16), ((0, 8), (0, 0)))
    keep = jnp.broadcast_to(onehot.astype(jnp.float32).reshape(SUBJ, -1, 1, GROUP),
                            (SUBJ, epochs // GROUP, SLOTS, GROUP)).reshape(SUBJ, span)
    squares, total = pl.pallas_call(
        features_kernel,
        grid=(block_len // CHUNK,),
        in_specs=[vmem] * 7,
        out_specs=[vmem] * 2,
        out_shape=[jax.ShapeDtypeStruct((block_len, epochs), jnp.float32),
                   jax.ShapeDtypeStruct((epochs, epochs), jnp.float32)],
        scratch_shapes=[
            pltpu.VMEM((2, span, wide), jnp.bfloat16),
            pltpu.VMEM((CHUNK * GROUP, depth), jnp.bfloat16),
            pltpu.VMEM((CHUNK, epochs, SPAN), jnp.float32),
            pltpu.VMEM((CHUNK, SUBJ, SPAN), jnp.float32),
            pltpu.VMEM((BATCH, epochs, SPAN), jnp.bfloat16),
            pltpu.VMEM((BATCH, epochs, SPAN), jnp.bfloat16),
            pltpu.VMEM((BATCH, SUBJ, SPAN), jnp.float32),
        ],
        compiler_params=pltpu.CompilerParams(dimension_semantics=("arbitrary",),
                                             vmem_limit_bytes=60 * 1024 * 1024),
        name="features",
    )(ext, own, root, sid, hot, inv, keep)
    spread = jnp.sqrt(jnp.sum(squares, axis=1) / (epochs * NB * NB))
    gram_mean = sum_over_bx(total, 1.0 / (NB * block_len * count))
    return spread, gram_mean


def solution(mesh):
    return jax.shard_map(
        per_device,
        mesh=mesh,
        in_specs=(P("cohort", None, "bx"), P("cohort", "bx"), P("cohort")),
        out_specs=(P(("cohort", "bx")), P("cohort", None)),
        check_vma=False,
    )
```
